512 devices in a mesh: seq: 16 (over z, core), exp: 32 (over y, x).
Axes of the slice: x: 4, y: 8, z: 8, core: 2. Of those that a mesh axis runs over, the one named last changes fastest.
Arguments:
- residual_in: bfloat16 [1024, 32, 1152], P('seq', 'exp'), may hold values from -6 to 6
- query_proj: bfloat16 [1024, 32, 1152], P('seq', 'exp'), may hold values from -6 to 6
- key_proj: bfloat16 [1024, 32, 1152], P('seq', 'exp'), may hold values from -6 to 6
- value_proj: bfloat16 [1024, 32, 1152], P('seq', 'exp'), may hold values from -6 to 6
- out_weight: bfloat16 [1152, 1152], replicated, may hold values from -0.1875 to 0.1875
- router_weight: bfloat16 [1152, 16], replicated, may hold values from -0.1875 to 0.1875
- first_weight: bfloat16 [32, 1152, 2304], P('exp', None, 'seq'), may hold values from -0.1875 to 0.1875
- second_weight: bfloat16 [32, 2304, 1152], P('exp', 'seq'), may hold values from -0.09375 to 0.09375
- class_table: bfloat16 [1024, 4, 1152], P('seq'), may hold values from -3 to 3
- time_weight: bfloat16 [256, 4, 1152], P('seq'), may hold values from -0.375 to 0.375
- class_labels: int32 [32], P('exp'), may hold values from 0 to 1023
- timesteps: int32 [32], P('exp'), may hold values from 0 to 999
- expert_ids: int32 [16, 32, 64, 1, 2], P('seq', 'exp'), may hold values from 0 to 15, all different within a row; in each aligned block of 64 rows (0 to 63, 64 to 127, ..., all dimensions but the last counted through in order) at most 10 rows name the same one
Outputs:
- block_out: bfloat16 [1024, 32, 1152], P('seq', 'exp')
The draws below stay inside these ranges and needn't reach their ends.
Inputs may be any that keep to these rules, and one draw needn't show every extreme that they name: `expert_ids`: each row names 2 different experts; among the rows of one device no expert is named by more than 10 rows.
All inputs are finite; a program needn't handle non-finite values.
Results may differ from the reference program's by a relative error of at most 0.013.
Values may be sent and summed in bfloat16 or wider, within the bound.
A program may use at most 64 MiB of HBM per device.

```python
import math
import jax
import jax.numpy as jnp
import numpy as np
from jax import lax

D = 1152
HEAD = 72
HEADS_WIN = 16
FFW = 4608
TOP = 2
FREQ = 256
CLASSES = 1024
LEN = 1024
IMG_DEV = 1
SEQ_DEV = 64
TOK_DEV = 64
IMAGES = 32
EXPERTS = 16
HW = 1152
CAP = 10
N_SEQ = 16
N_EXP = 32


def draw_key_proj(key, part):
    values = jnp.clip(jax.random.normal(jax.random.fold_in(key, 11), (LEN, IMAGES, HW), jnp.float32), -6.0, 6.0)
    return values.astype(jnp.bfloat16)


def draw_query_proj(key, part):
    values = jnp.clip(jax.random.normal(jax.random.fold_in(key, 21), (LEN, IMAGES, HW), jnp.float32), -6.0, 6.0)
    return values.astype(jnp.bfloat16)


def plant(values, key, low, high):
    shape = values.shape
    place = [jax.random.randint(jax.random.fold_in(key, axis), (), 0, shape[axis]) for axis in range(len(shape))]
    values = values.at[tuple(place)].set(low)
    longest = shape.index(max(shape))
    place[longest] = (place[longest] + 1) % shape[longest]
    return values.at[tuple(place)].set(high)


def steps_of(own_key, shape, shards, least, largest):
    def one(position, blocks):
        draws = jax.random.uniform(jax.random.fold_in(jax.random.fold_in(own_key, 6), position), (blocks,), jnp.float32, least / len(shards), largest / len(shards))
        return jnp.repeat(jnp.exp(draws), shape[position] // blocks).reshape((-1,) + (1,) * (len(shape) - position - 1))

    factor_of = one(*shards[0])
    for cut in shards[1:]:
        factor_of = factor_of * one(*cut)
    return factor_of


def routed_block(own_key, own, number, rows, number_of, top, limit, slope):
    order = jax.random.permutation(own_key, number_of)
    heavy_load, usual = load_shares(number_of, rows * top, limit, slope, True), load_shares(number_of, rows * top, limit, slope, False)
    places = jnp.arange(number_of)

    def named(lengths, turn):
        used = int((lengths > 0).sum())
        fixed = max(1, used // 4)
        passed = fixed + (places - fixed + turn * (used - fixed)) % max(1, number_of - fixed)
        return jnp.zeros((number_of,), jnp.int32).at[order[jnp.where(places < fixed, places, passed)]].set(jnp.asarray(lengths, jnp.int32))

    lengths = jnp.where(number % 4 == 0, named(heavy_load, number // 4), named(usual, number - number // 4 - 1))
    mixed = jax.random.permutation(jax.random.fold_in(own, 3), number_of)
    source_of, sink = mixed[0:number_of // 2 * 2:2], mixed[1:number_of // 2 * 2:2]
    margin = jnp.minimum(lengths[source_of] - 1, limit - lengths[sink]) // 2
    margin = jnp.where((source_of == order[0]) | (sink == order[0]) | (lengths[sink] == 0), 0, jnp.maximum(margin, 0))
    passed = jax.random.randint(jax.random.fold_in(own, 4), (number_of // 2,), 0, 1 << 20) % (margin + 1)
    lengths = lengths.at[source_of].add(-passed).at[sink].add(passed)
    items = jnp.searchsorted(jnp.cumsum(lengths), jnp.arange(rows * top), side="right").astype(jnp.int32)
    grid = items.reshape(top, rows).T
    grid = grid[jax.random.permutation(jax.random.fold_in(own, 1), rows)]
    turn = jax.random.randint(jax.random.fold_in(own, 2), (rows, 1), 0, top)
    return jnp.take_along_axis(grid, (jnp.arange(top)[None, :] + turn) % top, axis=1)


def load_shares(count, total, bound, skew, full):
    loads = [(1 << 20) // math.isqrt(rank ** skew) + 1 for rank in range(1, count + 1)]
    largest = bound if full else min(bound, max(-(-total // count), total * loads[0] // sum(loads)))
    least = 1 if total - largest >= count - 1 else 0
    given, surplus = [largest] + [least] * (count - 1), total - largest - least * (count - 1)
    while surplus > 0:
        movable = [i for i in range(1, count) if given[i] < largest] or [i for i in range(1, count) if given[i] < bound]
        mass, remaining = sum([loads[i] for i in movable]), surplus
        for i in movable:
            extra = min(bound - given[i], max(1, remaining * loads[i] // mass), surplus)
            given[i] = given[i] + extra
            surplus = surplus - extra
    return np.array(given)


def scatter_about(rng, extent, deviation, most, pieces=(), kind=jnp.bfloat16):
    loudness = steps_of(rng, extent, pieces, -0.22, 0.18) if pieces else 1.0
    values = jax.random.normal(rng, extent, jnp.float32) * deviation * loudness
    return jnp.minimum(jnp.maximum(values, -most), most).astype(kind)


def setup_inputs(seed: int = 0) -> dict:
    key_of = jax.random.split(jax.random.key(seed), 14)
    residual_in = scatter_about(key_of[0], (LEN, IMAGES, D), 1.0, 6.0, ((0, 16), (1, 32)))
    query_proj = draw_query_proj(jax.random.fold_in(key_of[13], 71), 0)
    key_proj = draw_key_proj(jax.random.fold_in(key_of[13], 71), 0)
    value_proj = scatter_about(key_of[3], (LEN, IMAGES, HW), 1.0, 6.0, ((0, 16), (1, 32)))
    out_weight = scatter_about(key_of[4], (HW, D), HW ** -0.5, 0.1875)
    router_weight = scatter_about(key_of[5], (D, EXPERTS), D ** -0.5, 0.1875)
    first_weight = scatter_about(key_of[6], (N_EXP, D, FFW // 2), D ** -0.5, 0.1875, ((0, 32), (2, 16)))
    second_weight = scatter_about(key_of[7], (N_EXP, FFW // 2, D), FFW ** -0.5, 0.09375, ((0, 32), (1, 16)))
    class_table = scatter_about(key_of[8], (CLASSES, 4, D), 0.5, 3.0, ((0, 16),))
    time_weight = scatter_about(key_of[9], (FREQ, 4, D), FREQ ** -0.5, 0.375, ((0, 16),))
    class_labels = plant(jax.random.randint(key_of[10], (IMAGES,), 0, CLASSES), jax.random.fold_in(key_of[10], 1), 0, CLASSES - 1).astype(jnp.int32)
    timesteps = plant(jax.random.randint(key_of[11], (IMAGES,), 0, 1000), jax.random.fold_in(key_of[11], 1), 0, 999).astype(jnp.int32)
    expert_ids_keys = jax.random.split(jax.random.fold_in(key_of[12], 1), N_SEQ * N_EXP * SEQ_DEV * IMG_DEV // TOK_DEV)
    expert_ids_turns = jax.random.permutation(jax.random.fold_in(key_of[12], 3), N_SEQ * N_EXP * SEQ_DEV * IMG_DEV // TOK_DEV)
    expert_ids = jax.vmap(lambda own, number: routed_block(jax.random.fold_in(key_of[12], 2), own, number, TOK_DEV, EXPERTS, TOP, CAP, 2))(expert_ids_keys, expert_ids_turns).reshape((N_SEQ, N_EXP, SEQ_DEV, IMG_DEV, TOP))
    return {"residual_in": residual_in, "query_proj": query_proj, "key_proj": key_proj, "value_proj": value_proj, "out_weight": out_weight, "router_weight": router_weight, "first_weight": first_weight, "second_weight": second_weight, "class_table": class_table, "time_weight": time_weight, "class_labels": class_labels, "timesteps": timesteps, "expert_ids": expert_ids}


def time_embed(timesteps):
    half_width = FREQ // 2
    frequencies = jnp.exp(-math.log(10000.0) * jnp.arange(half_width, dtype=jnp.float32) / half_width)
    angles = timesteps.astype(jnp.float32)[:, None] * frequencies[None, :]
    return jnp.concatenate([jnp.cos(angles), jnp.sin(angles)], axis=1)

def attend_image(operands):
    query_heads, key_heads, value_heads = operands
    inv_root = 1.0 / math.sqrt(HEAD)
    scores = jnp.einsum('qhe,khe->hqk', query_heads.astype(jnp.float32), key_heads.astype(jnp.float32)) * inv_root
    row_max = lax.optimization_barrier(jnp.max(scores, axis=-1, keepdims=True))
    exp_scores = jnp.exp(scores - row_max)
    row_total = lax.optimization_barrier(jnp.sum(exp_scores, axis=-1, keepdims=True))
    rounded_w = exp_scores.astype(jnp.bfloat16)
    mixed_out = jnp.einsum('hqk,khe->qhe', rounded_w.astype(jnp.float32), value_heads.astype(jnp.float32))
    return (mixed_out / jnp.transpose(row_total, (1, 0, 2))).astype(jnp.bfloat16)

def half_apply(block_rows, weight_one, weight_two):
    pre_act = jnp.dot(block_rows.astype(jnp.float32), weight_one.astype(jnp.float32), preferred_element_type=jnp.float32)
    inner_act = jax.nn.gelu(pre_act, approximate=True).astype(jnp.bfloat16)
    return jnp.dot(inner_act.astype(jnp.float32), weight_two.astype(jnp.float32), preferred_element_type=jnp.float32).astype(jnp.bfloat16)

def expert_apply(operands):
    block_rows, weight_one, weight_two = operands
    lower = half_apply(block_rows, weight_one[0], weight_two[0]).astype(jnp.float32)
    upper = half_apply(block_rows, weight_one[1], weight_two[1]).astype(jnp.float32)
    return (lower + upper).astype(jnp.bfloat16)

def to_blocks(array):
    tail = array.shape[2:]
    shaped = array.reshape((N_SEQ, LEN // N_SEQ, N_EXP, IMAGES // N_EXP) + tail)
    shaped = jnp.swapaxes(shaped, 1, 2)
    return shaped.reshape((N_SEQ * N_EXP, LEN // N_SEQ * (IMAGES // N_EXP)) + tail)

def from_blocks(array):
    tail = array.shape[2:]
    shaped = array.reshape((N_SEQ, N_EXP, LEN // N_SEQ, IMAGES // N_EXP) + tail)
    shaped = jnp.swapaxes(shaped, 1, 2)
    return shaped.reshape((LEN, IMAGES) + tail)

def reference(residual_in, query_proj, key_proj, value_proj, out_weight, router_weight, first_weight, second_weight, class_table, time_weight, class_labels, timesteps, expert_ids):
    table_rows = jnp.take(class_table, class_labels, axis=0).astype(jnp.float32)
    embedded = time_embed(timesteps)
    time_part = jnp.dot(embedded, time_weight.astype(jnp.float32).reshape(FREQ, 4 * D), precision=lax.Precision.HIGHEST)
    conditions = table_rows + time_part.reshape(IMAGES, 4, D)
    query_img = query_proj.reshape(LEN, IMAGES, HEADS_WIN, HEAD).transpose(1, 0, 2, 3)
    key_img = key_proj.reshape(LEN, IMAGES, HEADS_WIN, HEAD).transpose(1, 0, 2, 3)
    value_img = value_proj.reshape(LEN, IMAGES, HEADS_WIN, HEAD).transpose(1, 0, 2, 3)
    attended = lax.map(attend_image, (query_img, key_img, value_img))
    attended = attended.transpose(1, 0, 2, 3).reshape(LEN * IMAGES, HW)
    projected = jnp.dot(attended, out_weight, preferred_element_type=jnp.float32).reshape(LEN, IMAGES, D)
    updated = (residual_in.astype(jnp.float32) + conditions[None, :, 0, :] * projected).astype(jnp.bfloat16)
    updated_f = updated.astype(jnp.float32)
    mean_value = lax.optimization_barrier(jnp.mean(updated_f, axis=-1, keepdims=True))
    centered = updated_f - mean_value
    variance = lax.optimization_barrier(jnp.mean(centered * centered, axis=-1, keepdims=True))
    normed = centered * lax.rsqrt(variance + 1e-06)
    moe_in = (normed * (1.0 + conditions[None, :, 2, :]) + conditions[None, :, 1, :]).astype(jnp.bfloat16)
    logits = jnp.dot(moe_in.reshape(LEN * IMAGES, D), router_weight, preferred_element_type=jnp.float32)
    token_ids = jnp.swapaxes(expert_ids, 1, 2).reshape(LEN * IMAGES, TOP)
    chosen = jnp.take_along_axis(logits, token_ids, axis=1)
    first_share = jax.nn.sigmoid(chosen[:, 0] - chosen[:, 1]).reshape(LEN, IMAGES)
    block_count = N_SEQ * N_EXP
    blocks = expert_ids.reshape(block_count, -1)
    onehot = (blocks[:, :, None] == jnp.arange(EXPERTS, dtype=jnp.int32)[None, None, :]).astype(jnp.int32)
    slot_index = lax.optimization_barrier(jnp.sum(jnp.cumsum(onehot, axis=1) * onehot, axis=2)) - 1
    block_ids = jnp.arange(block_count, dtype=jnp.int32)[:, None]
    flat_index = (blocks * (block_count * CAP) + block_ids * CAP + slot_index).astype(jnp.int32).reshape(-1)
    block_rows = jnp.repeat(to_blocks(moe_in), TOP, axis=1).reshape(-1, D)
    buffer = jnp.zeros((EXPERTS * block_count * CAP, D), jnp.bfloat16).at[flat_index].set(block_rows)
    first_pairs = first_weight.reshape(EXPERTS, 2, D, FFW // 2)
    second_pairs = second_weight.reshape(EXPERTS, 2, FFW // 2, D)
    out_buffer = lax.map(expert_apply, (buffer.reshape(EXPERTS, block_count * CAP, D), first_pairs, second_pairs))
    returned = out_buffer.reshape(-1, D)[flat_index].reshape(block_count, -1, TOP, D).astype(jnp.float32)
    share_blocks = to_blocks(first_share[:, :, None])[:, :, 0]
    mixed_out = share_blocks[:, :, None] * returned[:, :, 0, :] + (1.0 - share_blocks)[:, :, None] * returned[:, :, 1, :]
    moe_out = from_blocks(mixed_out)
    return (updated_f + conditions[None, :, 3, :] * moe_out).astype(jnp.bfloat16)
```

```python
import functools
import math

import jax
import jax.numpy as jnp
from jax import lax
from jax.experimental import pallas as pl
from jax.experimental.pallas import tpu as pltpu
from jax.sharding import PartitionSpec as P

HEAD = 72
FREQ = 256
MESH = pl.DeviceIdType.MESH
NS = 16
NE = 32
NZ = 8
D = 1152
HID = 144
CAP = 10
PAD = 16
TILES = 9
NT = (((1,), (1,)), ((), ()))
NN = (((1,), (0,)), ((), ()))
F32 = jnp.float32
BF = jnp.bfloat16


def mm(a, b, dims=NN):
    return lax.dot_general(a, b, dims, preferred_element_type=F32)


def rcopy(src, dst, ssem, rsem, axis, peer):
    return pltpu.make_async_remote_copy(
        src_ref=src, dst_ref=dst, send_sem=ssem, recv_sem=rsem,
        device_id={axis: peer}, device_id_type=MESH,
    )


def kernel(
    q_ref, k_ref, v_ref, res_ref, ids_ref, label_ref, emb_ref, tw_ref, rt_ref,
    ct_hbm, wo_hbm, w1_hbm, w2_hbm, out_ref,
    qsend, qrecv, kk, vv, osend, orecv, att, ct, wo, cpart, crecv, cond,
    wbuf, moe_s, upd_s, wt, xsend, xrecv, acc, ysend, yrecv,
    q_ss, q_rs, o_ss, o_rs, c1_ss, c1_rs, c2_ss, c2_rs,
    cw_ss, ccw_ss, dd_ss, w_rs, x_ss, x_rs, y_ss, y_rs, l_s,
):
    s = lax.axis_index("seq")
    e = lax.axis_index("exp")
    z, c = s // 2, s % 2

    lw1 = pltpu.make_async_copy(w1_hbm, wbuf.at[s, 0], l_s.at[0])
    lw2 = pltpu.make_async_copy(w2_hbm, wbuf.at[s, 1], l_s.at[1])
    lct = pltpu.make_async_copy(ct_hbm, ct, l_s.at[2])
    lwo = pltpu.make_async_copy(wo_hbm, wo, l_s.at[3])
    lct.start()
    lw1.start()
    lw2.start()
    lwo.start()

    barrier = pltpu.get_barrier_semaphore()

    @pl.loop(1, NS)
    def _(d):
        pl.semaphore_signal(barrier, inc=1, device_id={"seq": (s + d) % NS}, device_id_type=MESH)

    @pl.loop(1, NE)
    def _(d):
        pl.semaphore_signal(barrier, inc=1, device_id={"exp": (e + d) % NE}, device_id_type=MESH)

    for h in range(NS):
        lanes = slice(h * HEAD, (h + 1) * HEAD)
        qsend[h, :, 0:HEAD] = q_ref[:, lanes]
        qsend[h, :, HEAD : 2 * HEAD] = k_ref[:, lanes]
        qsend[h, :, 2 * HEAD : 3 * HEAD] = v_ref[:, lanes]

    pl.semaphore_wait(barrier, NS - 1 + NE - 1)

    def qcopy(to, frm):
        return rcopy(qsend.at[to], qrecv.at[frm], q_ss.at[to], q_rs.at[frm], "seq", to)

    @pl.loop(1, NS)
    def _(d):
        qcopy((s + d) % NS, s).start()

    qrecv[s] = qsend[s]

    lct.wait()
    place = label_ref[0] - s * 64
    row = ct[jnp.clip(place, 0, 63)].astype(F32)
    part = jnp.where((place >= 0) & (place < 64), row, 0.0)
    for r in range(FREQ // NS):
        part = part + emb_ref[r] * tw_ref[r].astype(F32)
    for t in range(TILES):
        cpart[t] = part[:, t * 128 : (t + 1) * 128]

    def c1copy(to, frm):
        return rcopy(cpart.at[to], crecv.at[frm], c1_ss.at[to], c1_rs.at[frm], "seq", to)

    for t in range(TILES):
        @pl.when(s != t)
        def _(t=t):
            c1copy(t, s).start()

    @pl.when(s < TILES)
    def _():
        crecv[s] = cpart[s]

    @pl.loop(1, NS)
    def _(d):
        qcopy(s, (s + d) % NS).wait_recv()

    full = qrecv[...].reshape(NS * 64, 256)
    kk[...] = full[:, HEAD : 2 * HEAD]
    vv[...] = full[:, 2 * HEAD : 3 * HEAD]
    scale = 1.0 / math.sqrt(HEAD)

    def ocopy(to, frm):
        return rcopy(osend.at[to], orecv.at[frm], o_ss.at[to], o_rs.at[frm], "seq", to)

    @pl.loop(0, 4)
    def _(b):
        query = qrecv[pl.ds(b * 4, 4)].reshape(256, 256)[:, 0:HEAD]
        scores = mm(query, kk[...], NT) * scale
        top = jnp.max(scores, axis=-1, keepdims=True)
        w = jnp.exp(scores - top)
        total = jnp.sum(w, axis=-1, keepdims=True)
        o = mm(w.astype(BF), vv[...]) / total
        osend[pl.ds(b * 4, 4), :, 0:HEAD] = o.astype(BF).reshape(4, 64, HEAD)

        @pl.loop(0, 4)
        def _(i):
            j = b * 4 + i

            @pl.when(j != s)
            def _():
                ocopy(j, s).start()

    orecv[s] = osend[s]

    def ring(k, way, p):
        owner = (z + NZ - k) % NZ if way == 0 else (z + k) % NZ
        slot = owner * 2 + c
        to = ((z + 1) % NZ if way == 0 else (z + NZ - 1) % NZ) * 2 + c
        sems = cw_ss if way == 0 else ccw_ss
        return rcopy(wbuf.at[slot, p], wbuf.at[slot, p], sems.at[k, p], w_rs.at[slot, p], "seq", to)

    def arrival(k, way, p):
        owner = (z + 2 * NZ - 1 - k) % NZ if way == 0 else (z + 1 + k) % NZ
        slot = owner * 2 + c
        return rcopy(wbuf.at[slot, p], wbuf.at[slot, p], cw_ss.at[0, p], w_rs.at[slot, p], "seq", z * 2 + 1 - c)

    def across(owner, p, mine):
        slot = owner * 2 + (c if mine else 1 - c)
        return rcopy(wbuf.at[slot, p], wbuf.at[slot, p], dd_ss.at[owner, p], w_rs.at[slot, p], "seq", z * 2 + 1 - c)

    lw1.wait()
    lw2.wait()
    for p in range(2):
        ring(0, 0, p).start()
        ring(0, 1, p).start()
    for p in range(2):
        across(z, p, True).start()

    @pl.loop(0, NS)
    def _(i):
        @pl.when((s < TILES) & (i != s))
        def _():
            rcopy(cpart.at[0], crecv.at[i], c1_ss.at[0], c1_rs.at[i], "seq", (s + 1) % NS).wait_recv()

    def c2copy(tile, to):
        return rcopy(cond.at[tile], cond.at[tile], c2_ss.at[to], c2_rs.at[tile], "seq", to)

    @pl.when(s < TILES)
    def _():
        cond[s] = jnp.sum(crecv[...], axis=0)

        @pl.loop(1, NS)
        def _(d):
            c2copy(s, (s + d) % NS).start()

    ids0 = ids_ref[0:1, :]
    ids1 = ids_ref[1:2, :]
    rows = lax.broadcasted_iota(jnp.int32, (16 * PAD, 64), 0)
    of_e, of_s = rows // PAD, (rows % PAD).astype(F32)
    hit0, hit1 = ids0 == of_e, ids1 == of_e
    named = jnp.where(hit0 | hit1, 1.0, 0.0)
    earlier = jnp.where(
        lax.broadcasted_iota(jnp.int32, (64, 64), 0) < lax.broadcasted_iota(jnp.int32, (64, 64), 1), 1.0, 0.0
    )
    slot = mm(named.astype(BF), earlier.astype(BF))
    here = slot == of_s
    pick0 = jnp.where(hit0 & here, 1.0, 0.0)
    pick1 = jnp.where(hit1 & here, 1.0, 0.0)

    @pl.loop(1, NS)
    def _(d):
        ocopy(s, (s + d) % NS).wait_recv()

    for h in range(NS):
        att[:, h * HEAD : (h + 1) * HEAD] = orecv[h, :, 0:HEAD]
    lwo.wait()
    projected = mm(att[...], wo[...])

    for t in range(TILES):
        @pl.when(s != t)
        def _(t=t):
            c2copy(t, (s + 1) % NS).wait_recv()

    mods = jnp.concatenate([cond[t] for t in range(TILES)], axis=1)
    updated = (res_ref[...].astype(F32) + mods[0:1, :] * projected).astype(BF)
    upd_s[...] = updated
    updated_f = updated.astype(F32)
    mean = jnp.mean(updated_f, axis=-1, keepdims=True)
    centered = updated_f - mean
    variance = jnp.mean(centered * centered, axis=-1, keepdims=True)
    moe_in = (centered * lax.rsqrt(variance + 1e-6) * (1.0 + mods[2:3, :]) + mods[1:2, :]).astype(BF)

    xsend[...] = mm((pick0 + pick1).astype(BF), moe_in).astype(BF).reshape(16, PAD, D)

    def xcopy(to, frm):
        return rcopy(
            xsend.at[to // 2, pl.ds(0, ROWS)], xrecv.at[frm, pl.ds(0, ROWS)], x_ss.at[to], x_rs.at[frm], "exp", to
        )

    @pl.loop(1, NE)
    def _(d):
        xcopy((e + d) % NE, e).start()

    xrecv[e] = xsend[e // 2]

    logits = mm(rt_ref[...], moe_in, NT)
    experts = lax.broadcasted_iota(jnp.int32, (16, 64), 0)
    chosen0 = jnp.sum(jnp.where(experts == ids0, logits, 0.0), axis=0, keepdims=True)
    chosen1 = jnp.sum(jnp.where(experts == ids1, logits, 0.0), axis=0, keepdims=True)
    share = 1.0 / (1.0 + jnp.exp(-(chosen0 - chosen1)))
    weight = pick0 * share + pick1 * (1.0 - share)
    high = weight.astype(BF)
    low = (weight - high.astype(F32)).astype(BF)
    eye = jnp.where(
        lax.broadcasted_iota(jnp.int32, (64, 64), 0) == lax.broadcasted_iota(jnp.int32, (64, 64), 1), 1.0, 0.0
    ).astype(BF)
    wt[0] = mm(eye, high, NT).astype(BF)
    wt[1] = mm(eye, low, NT).astype(BF)

    def step(k, last):
        for p in range(2):
            for way in range(2):
                owner = (z + 2 * NZ - 1 - k) % NZ if way == 0 else (z + 1 + k) % NZ
                arrival(k, way, p).wait_recv()
                if last:
                    if way == p:
                        ring(k + 1, way, p).start()
                else:
                    ring(k + 1, way, p).start()
                across(owner, p, True).start()

    step(0, False)

    @pl.loop(1, NE)
    def _(d):
        xcopy(e, (e + d) % NE).wait_recv()

    def ffn(owner, first):
        across(owner, 0, False).wait_recv()
        across(owner, 1, False).wait_recv()
        w1 = wbuf[pl.ds(owner * 2, 2), 0].reshape(2 * HID, D)
        w2 = wbuf[pl.ds(owner * 2, 2), 1].reshape(2 * HID, D)
        for b in range(NB):
            x = xrecv[b * (NE // NB) : (b + 1) * (NE // NB)].reshape(NE // NB * PAD, D)
            hidden = jax.nn.gelu(mm(x, w1, NT), approximate=True).astype(BF)
            y = mm(hidden, w2)
            if first:
                acc[b] = y
            else:
                acc[b] = acc[b] + y

    ffn(z, True)

    @pl.loop(0, 3)
    def _(k):
        @pl.when(k > 0)
        def _():
            for p in range(2):
                for way in range(2):
                    owner = (z + 2 * NZ - 1 - k) % NZ if way == 0 else (z + 1 + k) % NZ
                    arrival(k, way, p).wait_recv()
                    if way == p:
                        ring(k + 1, way, p).start()
                    else:
                        @pl.when(k < 2)
                        def _():
                            ring(k + 1, way, p).start()
                    across(owner, p, True).start()

        @pl.loop(0, 2)
        def _(way):
            ffn(jnp.where(way == 0, (z + 2 * NZ - 1 - k) % NZ, (z + 1 + k) % NZ), False)

    far = (z + 4) % NZ
    arrival(3, 0, 0).wait_recv()
    across(far, 0, True).start()
    arrival(3, 1, 1).wait_recv()
    across(far, 1, True).start()
    across(far, 0, False).wait_recv()
    across(far, 1, False).wait_recv()
    w1 = wbuf[pl.ds(far * 2, 2), 0].reshape(2 * HID, D)
    w2 = wbuf[pl.ds(far * 2, 2), 1].reshape(2 * HID, D)

    def ycopy(to, frm):
        return rcopy(ysend.at[to, pl.ds(0, ROWS)], yrecv.at[frm, pl.ds(0, ROWS)], y_ss.at[to], y_rs.at[frm], "exp", to)

    @pl.loop(0, NB)
    def _(b):
        first = b * (NE // NB)
        x = xrecv[pl.ds(first, NE // NB)].reshape(NE // NB * PAD, D)
        hidden = jax.nn.gelu(mm(x, w1, NT), approximate=True).astype(BF)
        y = acc[b] + mm(hidden, w2)
        ysend[pl.ds(first, NE // NB)] = y.astype(BF).reshape(NE // NB, PAD, D)

        @pl.loop(0, NE // NB)
        def _(i):
            @pl.when(first + i != e)
            def _():
                ycopy(first + i, e).start()

    yrecv[e] = ysend[e]

    @pl.loop(1, NE)
    def _(d):
        ycopy(e, (e + d) % NE).wait_recv()

    halves = yrecv[...].reshape(16, 2, PAD, D)
    got = (halves[:, 0].astype(F32) + halves[:, 1].astype(F32)).reshape(16 * PAD, D)
    real = lax.broadcasted_iota(jnp.int32, (16 * PAD, 1), 0) % PAD < CAP
    got = jnp.where(real, got, 0.0).astype(BF)
    mixed = mm(wt[0], got) + mm(wt[1], got)
    gate = jnp.concatenate([cond[t] for t in range(TILES)], axis=1)[3:4, :]
    out_ref[...] = (upd_s[...].astype(F32) + gate * mixed).astype(BF)

    @pl.loop(1, NS)
    def _(d):
        qcopy((s + d) % NS, s).wait_send()
        ocopy((s + d) % NS, s).wait_send()

    for t in range(TILES):
        @pl.when(s != t)
        def _(t=t):
            c1copy(t, s).wait_send()

    @pl.when(s < TILES)
    def _():
        @pl.loop(1, NS)
        def _(d):
            c2copy(s, (s + d) % NS).wait_send()

    for k in range(4):
        for p in range(2):
            for way in range(2):
                if k < 3 or way == p:
                    ring(k, way, p).wait_send()

    @pl.loop(0, NZ)
    def _(i):
        across(i, 0, True).wait_send()
        across(i, 1, True).wait_send()

    @pl.loop(1, NE)
    def _(d):
        xcopy((e + d) % NE, e).wait_send()
        ycopy((e + d) % NE, e).wait_send()


ROWS = PAD
NB = 4


def body(
    residual_in, query_proj, key_proj, value_proj, out_weight, router_weight, first_weight, second_weight,
    class_table, time_weight, class_labels, timesteps, expert_ids,
):
    half = FREQ // 2
    index = lax.axis_index("seq") * (FREQ // NS) + jnp.arange(FREQ // NS, dtype=jnp.int32)
    frequency = jnp.exp(-math.log(10000.0) * (index % half).astype(F32) / half)
    angle = timesteps.astype(F32) * frequency
    emb = jnp.where(index < half, jnp.cos(angle), jnp.sin(angle))
    flat = lambda a: a.reshape(64, D)
    vmem = pl.BlockSpec(memory_space=pltpu.VMEM)
    smem = pl.BlockSpec(memory_space=pltpu.SMEM)
    anyspace = pl.BlockSpec(memory_space=pl.ANY)
    dma = pltpu.SemaphoreType.DMA
    out = pl.pallas_call(
        kernel,
        out_shape=jax.ShapeDtypeStruct((64, D), BF),
        in_specs=[vmem] * 5 + [smem] * 2 + [vmem] * 2 + [anyspace] * 4,
        out_specs=vmem,
        scratch_shapes=[
            pltpu.VMEM((NS, 64, 256), BF),
            pltpu.VMEM((NS, 64, 256), BF),
            pltpu.VMEM((NS * 64, HEAD), BF),
            pltpu.VMEM((NS * 64, HEAD), BF),
            pltpu.VMEM((NS, 64, 128), BF),
            pltpu.VMEM((NS, 64, 128), BF),
            pltpu.VMEM((64, D), BF),
            pltpu.VMEM((64, 4, D), BF),
            pltpu.VMEM((D, D), BF),
            pltpu.VMEM((TILES, 4, 128), F32),
            pltpu.VMEM((NS, 4, 128), F32),
            pltpu.VMEM((TILES, 4, 128), F32),
            pltpu.VMEM((NS, 2, HID, D), BF),
            pltpu.VMEM((64, D), BF),
            pltpu.VMEM((64, D), BF),
            pltpu.VMEM((2, 64, 16 * PAD), BF),
            pltpu.VMEM((16, PAD, D), BF),
            pltpu.VMEM((NE, PAD, D), BF),
            pltpu.VMEM((NB, NE // NB * PAD, D), F32),
            pltpu.VMEM((NE, PAD, D), BF),
            pltpu.VMEM((NE, PAD, D), BF),
            dma((NS,)), dma((NS,)), dma((NS,)), dma((NS,)),
            dma((TILES,)), dma((NS,)), dma((NS,)), dma((TILES,)),
            dma((4, 2)), dma((4, 2)), dma((NZ, 2)), dma((NS, 2)),
            dma((NE,)), dma((NE,)), dma((NE,)), dma((NE,)),
            dma((4,)),
        ],
        compiler_params=pltpu.CompilerParams(
            collective_id=0, has_side_effects=True, vmem_limit_bytes=58 * 1024 * 1024
        ),
    )(
        flat(query_proj), flat(key_proj), flat(value_proj), flat(residual_in),
        expert_ids.reshape(64, 2).T, class_labels, emb, time_weight, router_weight.T,
        class_table, out_weight, jnp.transpose(first_weight[0]), second_weight[0],
    )
    return out.reshape(64, 1, D)


def solution(mesh):
    return jax.shard_map(
        body,
        mesh=mesh,
        in_specs=(
            P("seq", "exp", None),
            P("seq", "exp", None),
            P("seq", "exp", None),
            P("seq", "exp", None),
            P(),
            P(),
            P("exp", None, "seq"),
            P("exp", "seq", None),
            P("seq", None, None),
            P("seq", None, None),
            P("exp"),
            P("exp"),
            P("seq", "exp", None, None, None),
        ),
        out_specs=P("seq", "exp", None),
        check_vma=False,
    )
```
